32 devices in a mesh: dp: 8 (over z, x), mp: 4 (over y, core).
Axes of the slice: x: 2, y: 2, z: 4, core: 2. Of those that a mesh axis runs over, the one named last changes fastest.
Arguments:
- inputs: bfloat16 [6144, 4608], P('dp'), may hold values from -8 to 8
- key_cotangent: bfloat16 [6144, 2048], P('dp', 'mp'), may hold values from -8 to 8
- master: float32 [4608, 2048], P('dp', 'mp'), may hold values from -0.09375 to 0.09375
- first_codes: int32 [4608, 2048], P('dp', 'mp'), may hold values from -127 to 127
- second_codes: int32 [4608, 2048], P('dp', 'mp'), may hold values from 1 to 255
- first_scale: float32 [1152, 4], P('dp', 'mp'), may hold values from 0.05 to 0.5
- second_scale: float32 [1152, 4], P('dp', 'mp'), may hold values from 0.02 to 0.2
Outputs:
- weight: bfloat16 [4608, 2048], P(None, 'mp')
- new_master: float32 [4608, 2048], P('dp', 'mp')
- first_unit: float32 [4608, 2048], P('dp', 'mp')
- second_unit: float32 [4608, 2048], P('dp', 'mp')
- first_top: float32 [1152, 4], P('dp', 'mp')
- second_top: float32 [1152, 4], P('dp', 'mp')
The draws below stay inside these ranges and needn't reach their ends.
All inputs are finite; a program needn't handle non-finite values. Where the reference program divides by a largest or mean magnitude, that divisor is 1e-20 or more.
Results may differ from the reference program's by a relative error of at most 0.0004.
Values may be sent and summed in bfloat16 or wider, within the bound.
A program may use at most 128 MiB of HBM per device.

```python
import math
import jax
import jax.numpy as jnp
from jax import lax

D = 4608
KV = 2048
QROWS = 4
QCOLS = 512
STEP = 10
TOKENS = 6144
N_DP = 8
N_MP = 4


def column_levels(key, width_total, groups):
    key_order, key_texture = jax.random.split(key, 2)
    ordering = jax.random.permutation(key_order, groups)
    ladder = jnp.exp(jnp.linspace(-0.6, 0.6, groups, dtype=jnp.float32))
    levels = ladder[ordering]
    texture = jax.random.uniform(key_texture, (width_total,), jnp.float32, minval=0.6, maxval=1.4)
    return jnp.repeat(levels, width_total // groups) * texture


def shaped_field(key, row_total, width_total, groups):
    key_level, key_main = jax.random.split(jax.random.fold_in(key, 17), 2)
    scales = column_levels(key_level, width_total, groups)
    normal_part = jax.random.normal(key_main, (row_total, width_total), jnp.float32)
    values = normal_part * scales[None, :]
    return jnp.clip(values, -8.0, 8.0).astype(jnp.bfloat16)


def draw_inputs(key, part):
    return shaped_field(jax.random.fold_in(key, 1), TOKENS, D, N_DP)


def draw_key_cotangent(key, part):
    return shaped_field(jax.random.fold_in(key, 2), TOKENS, KV, N_MP)


def set_ends(entries, own_key, smallest, high):
    index_at = [jax.random.randint(jax.random.fold_in(own_key, axis), (), 0, length) for axis, length in enumerate(entries.shape)]
    main_axis = entries.shape.index(max(entries.shape))
    beside = index_at[:main_axis] + [(index_at[main_axis] + 1) % entries.shape[main_axis]] + index_at[main_axis + 1:]
    return entries.at[tuple(index_at)].set(smallest).at[tuple(beside)].set(high)


def level_of(key, extent, shards, least, largest):
    gain, own = 1.0, jax.random.fold_in(key, 6)
    for dim, shards_of in shards:
        draws = jnp.exp(jax.random.uniform(jax.random.fold_in(own, dim), (shards_of,), jnp.float32, least / len(shards), largest / len(shards)))
        gain = gain * jnp.repeat(draws, extent[dim] // shards_of).reshape([-1 if axis == dim else 1 for axis in range(len(extent))])
    return gain


def centred(key, shape, width, reach, cuts=(), kind=jnp.bfloat16):
    drawn = width * jax.random.normal(key, shape, jnp.float32)
    if cuts:
        drawn = drawn * level_of(key, shape, cuts, -0.22, 0.18)
    return jnp.clip(drawn, -reach, reach).astype(kind)


def setup_inputs(seed: int = 0) -> dict:
    splits = jax.random.split(jax.random.key(seed), 8)
    return {
        "inputs": draw_inputs(jax.random.fold_in(splits[7], 71), 0),
        "key_cotangent": draw_key_cotangent(jax.random.fold_in(splits[7], 71), 0),
        "master": centred(splits[2], (D, KV), D ** -0.5, 0.09375, ((0, 8), (1, 4)), jnp.float32),
        "first_codes": set_ends(jax.random.randint(splits[3], (D, KV), -127, 128), jax.random.fold_in(splits[3], 1), -127, 127).astype(jnp.int32),
        "second_codes": set_ends(jax.random.randint(splits[4], (D, KV), 1, 256), jax.random.fold_in(splits[4], 1), 1, 255).astype(jnp.int32),
        "first_scale": jnp.clip(jnp.exp(math.log(0.5) - 2.3025851 * jax.random.uniform(splits[5], (D // QROWS, KV // QCOLS), jnp.float32) ** level_of(splits[5], (D // QROWS, KV // QCOLS), ((0, 8), (1, 4)), -0.2, 0.2)), 0.05, 0.5),
        "second_scale": jnp.clip(jnp.exp(math.log(0.2) - 2.3025851 * jax.random.uniform(splits[6], (D // QROWS, KV // QCOLS), jnp.float32) ** level_of(splits[6], (D // QROWS, KV // QCOLS), ((0, 8), (1, 4)), -0.2, 0.2)), 0.02, 0.2),
    }


beta_one = 0.9
beta_two = 0.95
learn_rate = 0.002
weight_decay = 0.1
epsilon = 1e-08
clip_rms = 0.25

def blocks(array):
    return array.reshape(array.shape[0] // QROWS, QROWS, array.shape[1] // QCOLS, QCOLS)

def adam_step(gradient, norm_sq, master, first_codes, second_codes, first_scale, second_scale):
    factor = jnp.minimum(1.0, clip_rms * math.sqrt(D * KV) / (jnp.sqrt(norm_sq) + 1e-06))
    clipped = blocks(gradient * factor)
    first_old = blocks(first_codes.astype(jnp.float32)) / 127.0 * first_scale[:, None, :, None]
    second_old = blocks(second_codes.astype(jnp.float32)) / 255.0 * second_scale[:, None, :, None]
    first_new = beta_one * first_old + (1.0 - beta_one) * clipped
    second_new = beta_two * second_old + (1.0 - beta_two) * clipped * clipped
    first_hat = first_new / (1.0 - beta_one ** STEP)
    second_hat = second_new / (1.0 - beta_two ** STEP)
    step_dir = (first_hat / (jnp.sqrt(second_hat) + epsilon)).reshape(master.shape)
    new_master = master - learn_rate * (step_dir + weight_decay * master)
    first_top = lax.optimization_barrier(jnp.max(jnp.abs(first_new), axis=(1, 3))) + 1e-06
    second_top = lax.optimization_barrier(jnp.max(second_new, axis=(1, 3))) + 1e-06
    first_unit = (first_new / first_top[:, None, :, None]).reshape(master.shape)
    second_unit = (second_new / second_top[:, None, :, None]).reshape(master.shape)
    return (new_master, first_unit, second_unit, first_top, second_top)

def reference(inputs, key_cotangent, master, first_codes, second_codes, first_scale, second_scale):
    gradient = lax.dot_general(inputs, key_cotangent, (((0,), (0,)), ((), ())), preferred_element_type=jnp.float32)
    norm_sq = jnp.sum(gradient * gradient)
    new_master, first_unit, second_unit, first_top, second_top = adam_step(gradient, norm_sq, master, first_codes, second_codes, first_scale, second_scale)
    weight = new_master.astype(jnp.bfloat16)
    return (weight, new_master, first_unit, second_unit, first_top, second_top)
```

```python
import functools
import math

import jax
import jax.numpy as jnp
from jax import lax
from jax.experimental import pallas as pl
from jax.experimental.pallas import tpu as pltpu
from jax.sharding import PartitionSpec as P

MESH = pl.DeviceIdType.MESH
QROWS = 4
STEP = 10
LANES = 128

beta_one = 0.9
beta_two = 0.95
learn_rate = 0.002
weight_decay = 0.1
epsilon = 1e-08
clip_rms = 0.25
CODE_MAX = 32767.0


def kernel(
    n,
    m,
    limit,
    x_hbm,
    cot_hbm,
    master_hbm,
    fc_hbm,
    sc_hbm,
    fscale_ref,
    sscale_ref,
    w_hbm,
    nm_hbm,
    fu_hbm,
    su_hbm,
    ftop_ref,
    stop_ref,
    x_v,
    cot_v,
    part,
    xs,
    xs_s,
    xr,
    xr_s,
    zs,
    zs_s,
    zr,
    zr_s,
    master,
    fc,
    sc,
    fn,
    sn,
    nm_v,
    fu_v,
    su_v,
    row1,
    row2,
    wbuf,
    nd_out,
    nd_in,
    nm_out,
    nm_in,
    in_sem,
    par_sem,
    xs_send,
    xs_recv,
    xss_send,
    xss_recv,
    zs_send,
    zs_recv,
    zss_send,
    zss_recv,
    nd_send,
    nd_recv,
    nmx_send,
    nmx_recv,
    wx_send,
    wx_recv,
    wz_send,
    wz_recv,
    wout_sem,
    out_sem,
):
    B = 2
    A = n // B
    rows, width = master.shape
    cols_total = x_v.shape[1]
    R = 96 if rows % 96 == 0 else rows
    NR = rows // R
    Q = rows // QROWS
    REP = width // LANES

    me = lax.axis_index("dp")
    my = lax.axis_index("mp")
    a = me // B
    b = me % B
    mate = a * B + (1 - b)

    hi = A - 1 - a
    lo = a
    up_longer = jnp.where(hi >= lo, 1, -1)
    short = jnp.minimum(hi, lo)
    long = jnp.maximum(hi, lo)

    def order(i):
        j = i - (long - short)
        d_far = long - i
        jj = jnp.maximum(j, 0)
        d_near = short - jj // 2
        sgn = jnp.where(jj % 2 == 0, up_longer, -up_longer)
        return jnp.where(j < 0, a + up_longer * d_far, a + sgn * d_near)

    per_chunk = (B * rows) % 384 == 0
    csize = B * rows

    def in_copy(c):
        if per_chunk:
            sl = pl.ds(pl.multiple_of(c * csize, LANES), csize)
            return pltpu.make_async_copy(x_hbm.at[:, sl], x_v.at[:, sl], in_sem.at[c])
        return pltpu.make_async_copy(x_hbm, x_v, in_sem.at[0])

    cot_copy = pltpu.make_async_copy(cot_hbm, cot_v, par_sem.at[0])
    par_copies = [
        pltpu.make_async_copy(src, dst, par_sem.at[k + 1])
        for k, (src, dst) in enumerate(((master_hbm, master), (fc_hbm, fc), (sc_hbm, sc)))
    ]
    cot_copy.start()
    if per_chunk:

        @pl.loop(0, A)
        def _(i):
            in_copy(order(i)).start()
    else:
        in_copy(0).start()
    for cp in par_copies:
        cp.start()

    barrier = pltpu.get_barrier_semaphore()

    @pl.loop(1, n)
    def _(k):
        pl.semaphore_signal(barrier, inc=1, device_id={"dp": (me + k) % n}, device_id_type=MESH)

    @pl.loop(1, m)
    def _(k):
        pl.semaphore_signal(barrier, inc=1, device_id={"mp": (my + k) % m}, device_id_type=MESH)

    def multiply(first, count):
        @pl.loop(0, count)
        def _(k):
            at = pl.ds(pl.multiple_of(first + k * 384, LANES), 384)
            part[at, :] = lax.dot_general(
                x_v[:, at], cot_v[...], (((0,), (0,)), ((), ())), preferred_element_type=jnp.float32
            )

    def at_rows(block, r):
        return pl.ds(pl.multiple_of(block * rows + r * R, 8), R)

    def chunk_rows(r):
        return pl.ds(pl.multiple_of(r * R, 8), R)

    def fold(v):
        return v.reshape(R // 8, 8, width)

    def encode(block, dst, dst_s, top):
        top = jnp.maximum(top, 1e-30)
        dst_s[...] = top * (1.0 / CODE_MAX)
        inv = (CODE_MAX / top)[None]

        @pl.loop(0, NR)
        def _(r):
            v = jnp.round(fold(part[at_rows(block, r), :]) * inv).reshape(R, width)
            dst[chunk_rows(r), :] = v.astype(jnp.int32).astype(jnp.int16)

    def top_of(block):
        def body(r, t):
            return jnp.maximum(t, jnp.max(jnp.abs(fold(part[at_rows(block, r), :])), axis=0))

        return lax.fori_loop(0, NR, body, jnp.zeros((8, width), jnp.float32))

    def add(block, src, src_s):
        s = src_s[...][None]

        @pl.loop(0, NR)
        def _(r):
            v = fold(src[chunk_rows(r), :].astype(jnp.int32).astype(jnp.float32)) * s
            part[at_rows(block, r), :] = part[at_rows(block, r), :] + v.reshape(R, width)

    def pair_copies(c):
        to = {"dp": mate}
        return (
            pltpu.make_async_remote_copy(
                xs.at[c], xr.at[c], xs_send.at[c], xs_recv.at[c], device_id=to, device_id_type=MESH
            ),
            pltpu.make_async_remote_copy(
                xs_s.at[c], xr_s.at[c], xss_send.at[c], xss_recv.at[c], device_id=to, device_id_type=MESH
            ),
        )

    def line_copies(c, slot, to):
        to = {"dp": to}
        return (
            pltpu.make_async_remote_copy(
                zs.at[c], zr.at[slot], zs_send.at[c], zs_recv.at[slot], device_id=to, device_id_type=MESH
            ),
            pltpu.make_async_remote_copy(
                zs_s.at[c], zr_s.at[slot], zss_send.at[c], zss_recv.at[slot], device_id=to, device_id_type=MESH
            ),
        )

    cot_copy.wait()
    if not per_chunk:
        in_copy(0).wait()
        multiply(0, cols_total // 384)

    @pl.loop(0, A)
    def _(i):
        c = order(i)
        if per_chunk:
            in_copy(c).wait()
            multiply(c * csize, csize // 384)
        block = c * B + (1 - b)
        encode(block, xs.at[c], xs_s.at[c], top_of(block))

        @pl.when(i == 0)
        def _():
            pl.semaphore_wait(barrier, n - 1 + m - 1)

        for cp in pair_copies(c):
            cp.start()

    def receive(c, slot):
        for cp in line_copies(c, slot, me):
            cp.wait_recv()
        add(c * B + b, zr.at[slot], zr_s.at[slot])

    def forward(c, slot, to):
        block = c * B + b
        encode(block, zs.at[c], zs_s.at[c], top_of(block))
        for cp in line_copies(c, slot, to):
            cp.start()

    @pl.loop(0, A)
    def _(i):
        c = order(i)
        for cp in pair_copies(c):
            cp.wait_recv()
        add(c * B + b, xr.at[c], xr_s.at[c])

        @pl.when((c >= a) & (a > 0))
        def _():
            receive(c, c)

        @pl.when((c <= a) & (a < A - 1))
        def _():
            receive(c, A + c)

        @pl.when(c > a)
        def _():
            forward(c, c, me + B)

        @pl.when(c < a)
        def _():
            forward(c, A + c, me - B)

    def square(r, t):
        g = fold(part[at_rows(me, r), :])
        return t + jnp.sum(g * g, axis=0)

    squares = lax.fori_loop(0, NR, square, jnp.zeros((8, width), jnp.float32))
    mine = squares[:, :LANES]
    for k in range(1, REP):
        mine = mine + squares[:, k * LANES : (k + 1) * LANES]

    def exchange(axis, size, own, value, out, inbox, send, recv):
        out[...] = value
        inbox[own] = value

        def copy(k, slot):
            return pltpu.make_async_remote_copy(
                out,
                inbox.at[slot],
                send.at[k],
                recv.at[slot],
                device_id={axis: (own + k) % size},
                device_id_type=MESH,
            )

        @pl.loop(1, size)
        def _(k):
            copy(k, own).start()

        @pl.loop(1, size)
        def _(k):
            copy(k, (own + k) % size).wait_recv()

        @pl.loop(1, size)
        def _(k):
            copy(k, own).wait_send()

        return jnp.sum(inbox[...], axis=0)

    over_dp = exchange("dp", n, me, mine, nd_out, nd_in, nd_send, nd_recv)
    over_all = exchange("mp", m, my, over_dp, nm_out, nm_in, nmx_send, nmx_recv)
    norm_sq = jnp.sum(jnp.sum(over_all, axis=0, keepdims=True), axis=1, keepdims=True)
    factor = jnp.minimum(1.0, limit / (jnp.sqrt(norm_sq) + 1e-06))

    for cp in par_copies:
        cp.wait()
    for j in range(QROWS):
        every = pl.ds(j, Q, stride=QROWS)
        row1[every, :] = jnp.broadcast_to(fscale_ref[...] * (1.0 / 127.0), (Q, LANES))
        row2[every, :] = jnp.broadcast_to(sscale_ref[...] * (1.0 / 255.0), (Q, LANES))

    def wide(v):
        return jnp.concatenate([v] * REP, axis=1)

    @pl.loop(0, NR)
    def _(r):
        at = chunk_rows(r)
        clipped = part[at_rows(me, r), :] * factor
        first_new = beta_one * (fc[at, :].astype(jnp.float32) * wide(row1[at, :])) + (1.0 - beta_one) * clipped
        second_new = (
            beta_two * (sc[at, :].astype(jnp.float32) * wide(row2[at, :])) + (1.0 - beta_two) * clipped * clipped
        )
        fn[at, :] = first_new
        sn[at, :] = second_new
        first_hat = first_new * (1.0 / (1.0 - beta_one**STEP))
        second_hat = second_new * (1.0 / (1.0 - beta_two**STEP))
        step_dir = first_hat / (jnp.sqrt(second_hat) + epsilon)
        old = master[at, :]
        new = old - learn_rate * (step_dir + weight_decay * old)
        nm_v[at, :] = new
        wbuf[me, at, :] = new.astype(jnp.bfloat16)

    def pair_weight(c, block):
        return pltpu.make_async_remote_copy(
            wbuf.at[block],
            wbuf.at[block],
            wx_send.at[c],
            wx_recv.at[c],
            device_id={"dp": mate},
            device_id_type=MESH,
        )

    def line_weight(c, way, to):
        block = c * B + b
        return pltpu.make_async_remote_copy(
            wbuf.at[block],
            wbuf.at[block],
            wz_send.at[way * A + c],
            wz_recv.at[c],
            device_id={"dp": to},
            device_id_type=MESH,
        )

    def weight_out(block):
        return pltpu.make_async_copy(wbuf.at[block], w_hbm.at[block], wout_sem.at[block])

    @pl.when(a < A - 1)
    def _():
        line_weight(a, 0, me + B).start()

    @pl.when(a > 0)
    def _():
        line_weight(a, 1, me - B).start()

    pair_weight(a, me).start()
    weight_out(me).start()
    nm_out_copy = pltpu.make_async_copy(nm_v, nm_hbm, out_sem.at[0])
    fu_out_copy = pltpu.make_async_copy(fu_v, fu_hbm, out_sem.at[1])
    su_out_copy = pltpu.make_async_copy(su_v, su_hbm, out_sem.at[2])
    nm_out_copy.start()

    @pl.loop(0, NR)
    def _(r):
        at = chunk_rows(r)
        row1[at, :] = jnp.broadcast_to(jnp.max(jnp.abs(fn[at, :]), axis=1, keepdims=True), (R, LANES))
        row2[at, :] = jnp.broadcast_to(jnp.max(sn[at, :], axis=1, keepdims=True), (R, LANES))

    for row, top_ref in ((row1, ftop_ref), (row2, stop_ref)):
        top = row[pl.ds(0, Q, stride=QROWS), :]
        for j in range(1, QROWS):
            top = jnp.maximum(top, row[pl.ds(j, Q, stride=QROWS), :])
        top = top + 1e-06
        top_ref[...] = top[:, :1]
        for j in range(QROWS):
            row[pl.ds(j, Q, stride=QROWS), :] = 1.0 / top

    @pl.loop(0, NR)
    def _(r):
        at = chunk_rows(r)
        fu_v[at, :] = fn[at, :] * wide(row1[at, :])
        su_v[at, :] = sn[at, :] * wide(row2[at, :])

    fu_out_copy.start()
    su_out_copy.start()

    @pl.loop(1, A)
    def _(d):
        @pl.when(a - d >= 0)
        def _():
            c = a - d
            line_weight(c, 0, me).wait_recv()

            @pl.when(a < A - 1)
            def _():
                line_weight(c, 0, me + B).start()

            pair_weight(c, c * B + b).start()
            weight_out(c * B + b).start()

        @pl.when(a + d < A)
        def _():
            c = a + d
            line_weight(c, 1, me).wait_recv()

            @pl.when(a > 0)
            def _():
                line_weight(c, 1, me - B).start()

            pair_weight(c, c * B + b).start()
            weight_out(c * B + b).start()

        @pl.when(d == 1)
        def _():
            pair_weight(a, mate).wait_recv()
            weight_out(mate).start()

    @pl.loop(1, A)
    def _(d):
        @pl.when(a - d >= 0)
        def _():
            c = a - d
            pair_weight(c, c * B + 1 - b).wait_recv()
            weight_out(c * B + 1 - b).start()

        @pl.when(a + d < A)
        def _():
            c = a + d
            pair_weight(c, c * B + 1 - b).wait_recv()
            weight_out(c * B + 1 - b).start()

    @pl.loop(0, A)
    def _(c):
        for cp in pair_copies(c):
            cp.wait_send()

        @pl.when(c != a)
        def _():
            for cp in line_copies(c, c, me):
                cp.wait_send()

        pair_weight(c, c * B + b).wait_send()

        @pl.when((c <= a) & (a < A - 1))
        def _():
            line_weight(c, 0, me).wait_send()

        @pl.when((c >= a) & (a > 0))
        def _():
            line_weight(c, 1, me).wait_send()

    @pl.loop(0, n)
    def _(k):
        weight_out(k).wait()

    nm_out_copy.wait()
    fu_out_copy.wait()
    su_out_copy.wait()


def shards(n, m, limit, inputs, key_cotangent, master, first_codes, second_codes, first_scale, second_scale):
    rows, width = master.shape
    tokens, cols = inputs.shape
    A = n // 2
    f32 = jnp.float32
    any_spec = pl.BlockSpec(memory_space=pl.ANY)
    vmem_spec = pl.BlockSpec(memory_space=pltpu.VMEM)
    dma = pltpu.SemaphoreType.DMA
    block = (rows, width)
    outs = pl.pallas_call(
        functools.partial(kernel, n, m, limit),
        out_shape=(
            jax.ShapeDtypeStruct((n, rows, width), jnp.bfloat16),
            jax.ShapeDtypeStruct(block, f32),
            jax.ShapeDtypeStruct(block, f32),
            jax.ShapeDtypeStruct(block, f32),
            jax.ShapeDtypeStruct(first_scale.shape, f32),
            jax.ShapeDtypeStruct(second_scale.shape, f32),
        ),
        in_specs=[any_spec] * 5 + [vmem_spec] * 2,
        out_specs=[any_spec] * 4 + [vmem_spec] * 2,
        scratch_shapes=[
            pltpu.VMEM((tokens, cols), jnp.bfloat16),
            pltpu.VMEM(key_cotangent.shape, jnp.bfloat16),
            pltpu.VMEM((cols, width), f32),
            pltpu.VMEM((A, rows, width), jnp.int16),
            pltpu.VMEM((A, 8, width), f32),
            pltpu.VMEM((A, rows, width), jnp.int16),
            pltpu.VMEM((A, 8, width), f32),
            pltpu.VMEM((A, rows, width), jnp.int16),
            pltpu.VMEM((A, 8, width), f32),
            pltpu.VMEM((2 * A, rows, width), jnp.int16),
            pltpu.VMEM((2 * A, 8, width), f32),
            pltpu.VMEM(block, f32),
            pltpu.VMEM(block, jnp.int32),
            pltpu.VMEM(block, jnp.int32),
            pltpu.VMEM(block, f32),
            pltpu.VMEM(block, f32),
            pltpu.VMEM(block, f32),
            pltpu.VMEM(block, f32),
            pltpu.VMEM(block, f32),
            pltpu.VMEM((rows, LANES), f32),
            pltpu.VMEM((rows, LANES), f32),
            pltpu.VMEM((n, rows, width), jnp.bfloat16),
            pltpu.VMEM((8, LANES), f32),
            pltpu.VMEM((n, 8, LANES), f32),
            pltpu.VMEM((8, LANES), f32),
            pltpu.VMEM((m, 8, LANES), f32),
            dma((A,)),
            dma((4,)),
            dma((A,)),
            dma((A,)),
            dma((A,)),
            dma((A,)),
            dma((A,)),
            dma((2 * A,)),
            dma((A,)),
            dma((2 * A,)),
            dma((n,)),
            dma((n,)),
            dma((m,)),
            dma((m,)),
            dma((A,)),
            dma((A,)),
            dma((2 * A,)),
            dma((A,)),
            dma((n,)),
            dma((3,)),
        ],
        compiler_params=pltpu.CompilerParams(
            collective_id=0, has_side_effects=True, vmem_limit_bytes=62 * 1024 * 1024
        ),
        name="step",
    )(inputs, key_cotangent, master, first_codes, second_codes, first_scale, second_scale)
    weight = outs[0].reshape(n * rows, width)
    return (weight, *outs[1:])


def solution(mesh):
    n, m = mesh.shape["dp"], mesh.shape["mp"]

    def run(inputs, key_cotangent, master, *rest):
        limit = clip_rms * math.sqrt(inputs.shape[1] * key_cotangent.shape[1])
        return jax.shard_map(
            functools.partial(shards, n, m, limit),
            mesh=mesh,
            in_specs=(
                P("dp", None),
                P("dp", "mp"),
                P("dp", "mp"),
                P("dp", "mp"),
                P("dp", "mp"),
                P("dp", "mp"),
                P("dp", "mp"),
            ),
            out_specs=(
                P(None, "mp"),
                P("dp", "mp"),
                P("dp", "mp"),
                P("dp", "mp"),
                P("dp", "mp"),
                P("dp", "mp"),
            ),
            check_vma=False,
        )(inputs, key_cotangent, master, *rest)

    return run
```

```python
import functools
import math

import jax
import jax.numpy as jnp
from jax import lax
from jax.experimental import pallas as pl
from jax.experimental.pallas import tpu as pltpu
from jax.sharding import PartitionSpec as P

MESH = pl.DeviceIdType.MESH
QROWS = 4
STEP = 10
LANES = 128

beta_one = 0.9
beta_two = 0.95
learn_rate = 0.002
weight_decay = 0.1
epsilon = 1e-08
clip_rms = 0.25
CODE_MAX = 32767.0


def kernel(
    n,
    m,
    limit,
    x_hbm,
    cot_hbm,
    master_hbm,
    fc_hbm,
    sc_hbm,
    fscale_ref,
    sscale_ref,
    w_hbm,
    nm_hbm,
    fu_hbm,
    su_hbm,
    ftop_ref,
    stop_ref,
    x_v,
    cot_v,
    part,
    xs,
    xs_s,
    xr,
    xr_s,
    zs,
    zs_s,
    zr,
    zr_s,
    zts,
    zts_s,
    ztr,
    ztr_s,
    xt,
    xt_s,
    master,
    fc,
    sc,
    fn,
    sn,
    nm_v,
    fu_v,
    su_v,
    row1,
    row2,
    wbuf,
    nd_out,
    nd_in,
    nm_out,
    nm_in,
    in_sem,
    par_sem,
    xs_send,
    xs_recv,
    xss_send,
    xss_recv,
    zs_send,
    zs_recv,
    zss_send,
    zss_recv,
    zt_send,
    zt_recv,
    xt_sem,
    nd_send,
    nd_recv,
    nmx_send,
    nmx_recv,
    wx_send,
    wx_recv,
    wz_send,
    wz_recv,
    wxt_sem,
    wt_send,
    wt_recv,
    wout_sem,
    out_sem,
):
    B = 2
    A = n // B
    rows, width = master.shape
    cols_total = x_v.shape[1]
    R = 96 if rows % 96 == 0 else rows
    NR = rows // R
    NT = 1 if NR >= 6 else 0
    NM = NR - NT
    tail = NM
    Q = rows // QROWS
    REP = width // LANES

    me = lax.axis_index("dp")
    my = lax.axis_index("mp")
    a = me // B
    b = me % B
    mate = a * B + (1 - b)

    hi = A - 1 - a
    lo = a
    up_longer = jnp.where(hi >= lo, 1, -1)
    short = jnp.minimum(hi, lo)
    long = jnp.maximum(hi, lo)

    def order(i):
        j = i - (long - short)
        d_far = long - i
        jj = jnp.maximum(j, 0)
        d_near = short - jj // 2
        sgn = jnp.where(jj % 2 == 0, up_longer, -up_longer)
        return jnp.where(j < 0, a + up_longer * d_far, a + sgn * d_near)

    per_chunk = (B * rows) % 384 == 0
    csize = B * rows

    def in_copy(c):
        if per_chunk:
            sl = pl.ds(pl.multiple_of(c * csize, LANES), csize)
            return pltpu.make_async_copy(x_hbm.at[:, sl], x_v.at[:, sl], in_sem.at[c])
        return pltpu.make_async_copy(x_hbm, x_v, in_sem.at[0])

    cot_copy = pltpu.make_async_copy(cot_hbm, cot_v, par_sem.at[0])
    par_copies = [
        pltpu.make_async_copy(src, dst, par_sem.at[k + 1])
        for k, (src, dst) in enumerate(((master_hbm, master), (fc_hbm, fc), (sc_hbm, sc)))
    ]
    cot_copy.start()
    if per_chunk:

        @pl.loop(0, A)
        def _(i):
            in_copy(order(i)).start()
    else:
        in_copy(0).start()
    for cp in par_copies:
        cp.start()

    barrier = pltpu.get_barrier_semaphore()

    @pl.loop(1, n)
    def _(k):
        pl.semaphore_signal(barrier, inc=1, device_id={"dp": (me + k) % n}, device_id_type=MESH)

    @pl.loop(1, m)
    def _(k):
        pl.semaphore_signal(barrier, inc=1, device_id={"mp": (my + k) % m}, device_id_type=MESH)

    def multiply(first, count):
        @pl.loop(0, count)
        def _(k):
            at = pl.ds(pl.multiple_of(first + k * 384, LANES), 384)
            part[at, :] = lax.dot_general(
                x_v[:, at], cot_v[...], (((0,), (0,)), ((), ())), preferred_element_type=jnp.float32
            )

    def at_rows(block, r):
        return pl.ds(pl.multiple_of(block * rows + r * R, 8), R)

    def chunk_rows(r):
        return pl.ds(pl.multiple_of(r * R, 8), R)

    def fold(v):
        return v.reshape(R // 8, 8, width)

    def encode(block, r, dst, dst_s):
        v = fold(part[at_rows(block, r), :])
        top = jnp.maximum(jnp.max(jnp.abs(v), axis=0), 1e-30)
        dst_s[...] = top * (1.0 / CODE_MAX)
        v = jnp.round(v * (CODE_MAX / top)[None]).reshape(R, width)
        dst[...] = v.astype(jnp.int32).astype(jnp.int16)

    def decode(src, src_s):
        return fold(src[...].astype(jnp.int32).astype(jnp.float32)) * src_s[...][None]

    def add(block, r, src, src_s):
        at = at_rows(block, r)
        part[at, :] = part[at, :] + decode(src, src_s).reshape(R, width)

    def remote(src, dst, send, recv, **to):
        return pltpu.make_async_remote_copy(src, dst, send, recv, device_id=to, device_id_type=MESH)

    def pair_copies(c, r):
        k = c * NM + r
        return (
            remote(xs.at[k], xr.at[k], xs_send.at[k], xs_recv.at[k], dp=mate),
            remote(xs_s.at[k], xr_s.at[k], xss_send.at[k], xss_recv.at[k], dp=mate),
        )

    def line_copies(c, r, way, to):
        k = c * NM + r
        t = (way * A + c) * NM + r
        return (
            remote(zs.at[k], zr.at[t], zs_send.at[k], zs_recv.at[t], dp=to),
            remote(zs_s.at[k], zr_s.at[t], zss_send.at[k], zss_recv.at[t], dp=to),
        )

    def tail_copies(c, half, way, to):
        k = c * B + half
        t = (way * A + c) * B + half
        return (
            remote(zts.at[k], ztr.at[t], zt_send.at[0, k], zt_recv.at[0, t], dp=to),
            remote(zts_s.at[k], ztr_s.at[t], zt_send.at[1, k], zt_recv.at[1, t], dp=to),
        )

    pair_tail = (
        remote(xt.at[0], xt.at[1], xt_sem.at[0], xt_sem.at[1], dp=mate),
        remote(xt_s.at[0], xt_s.at[1], xt_sem.at[2], xt_sem.at[3], dp=mate),
    )

    cot_copy.wait()
    if not per_chunk:
        in_copy(0).wait()
        multiply(0, cols_total // 384)

    def send_tail(c):
        for way, on, to in ((0, c > a, me + B), (1, c < a, me - B)):

            @pl.when(on)
            def _():
                for half in range(B):
                    k = c * B + half
                    encode(k, tail, zts.at[k], zts_s.at[k])
                    for cp in tail_copies(c, half, way, to):
                        cp.start()

    def receive_tail(c, way):
        for half in range(B):
            t = (way * A + c) * B + half
            for cp in tail_copies(c, half, way, me):
                cp.wait_recv()
            add(c * B + half, tail, ztr.at[t], ztr_s.at[t])

    def starts(c):
        return ((c > a) & (a == 0)) | ((c < a) & (a == A - 1))

    @pl.loop(0, A)
    def _(i):
        c = order(i)
        if per_chunk:
            in_copy(c).wait()
            multiply(c * csize, csize // 384)
        block = c * B + (1 - b)

        @pl.when(i == 0)
        def _():
            pl.semaphore_wait(barrier, n - 1 + m - 1)

        @pl.loop(0, NM)
        def _(r):
            k = c * NM + r
            encode(block, r, xs.at[k], xs_s.at[k])
            for cp in pair_copies(c, r):
                cp.start()

        if NT:

            @pl.when(starts(c))
            def _():
                send_tail(c)

    def receive(c, r, way):
        t = (way * A + c) * NM + r
        for cp in line_copies(c, r, way, me):
            cp.wait_recv()
        add(c * B + b, r, zr.at[t], zr_s.at[t])

    def forward(c, r, way, to):
        k = c * NM + r
        encode(c * B + b, r, zs.at[k], zs_s.at[k])
        for cp in line_copies(c, r, way, to):
            cp.start()

    @pl.loop(0, A)
    def _(i):
        c = order(i)
        if NT:
            for way, on in ((0, (c >= a) & (a > 0)), (1, (c <= a) & (a < A - 1))):

                @pl.when(on)
                def _():
                    receive_tail(c, way)

            @pl.when((c != a) & jnp.logical_not(starts(c)))
            def _():
                send_tail(c)

            @pl.when(c == a)
            def _():
                encode(mate, tail, xt.at[0], xt_s.at[0])
                for cp in pair_tail:
                    cp.start()

        @pl.loop(0, NM)
        def _(r):
            k = c * NM + r
            for cp in pair_copies(c, r):
                cp.wait_recv()
            add(c * B + b, r, xr.at[k], xr_s.at[k])

            for way, on in ((0, (c >= a) & (a > 0)), (1, (c <= a) & (a < A - 1))):

                @pl.when(on)
                def _():
                    receive(c, r, way)

            for way, on, to in ((0, c > a, me + B), (1, c < a, me - B)):

                @pl.when(on)
                def _():
                    forward(c, r, way, to)

    if NT:
        for cp in pair_tail:
            cp.wait_recv()
        add(me, tail, xt.at[1], xt_s.at[1])

    def square(r, t):
        g = fold(part[at_rows(me, r), :])
        return t + jnp.sum(g * g, axis=0)

    squares = lax.fori_loop(0, NR, square, jnp.zeros((8, width), jnp.float32))
    mine = squares[:, :LANES]
    for k in range(1, REP):
        mine = mine + squares[:, k * LANES : (k + 1) * LANES]

    def exchange(axis, size, own, value, out, inbox, send, recv):
        out[...] = value
        inbox[own] = value

        def copy(k, slot):
            return pltpu.make_async_remote_copy(
                out,
                inbox.at[slot],
                send.at[k],
                recv.at[slot],
                device_id={axis: (own + k) % size},
                device_id_type=MESH,
            )

        @pl.loop(1, size)
        def _(k):
            copy(k, own).start()

        @pl.loop(1, size)
        def _(k):
            copy(k, (own + k) % size).wait_recv()

        @pl.loop(1, size)
        def _(k):
            copy(k, own).wait_send()

        return jnp.sum(inbox[...], axis=0)

    over_dp = exchange("dp", n, me, mine, nd_out, nd_in, nd_send, nd_recv)
    over_all = exchange("mp", m, my, over_dp, nm_out, nm_in, nmx_send, nmx_recv)
    norm_sq = jnp.sum(jnp.sum(over_all, axis=0, keepdims=True), axis=1, keepdims=True)
    factor = jnp.minimum(1.0, limit / (jnp.sqrt(norm_sq) + 1e-06))

    for cp in par_copies:
        cp.wait()
    pick = lax.broadcasted_iota(jnp.int32, (Q, Q), 0) == lax.broadcasted_iota(jnp.int32, (Q, Q), 1)

    def column(row):
        return jnp.sum(jnp.where(pick, row, 0.0), axis=1, keepdims=True)

    for j in range(QROWS):
        every = pl.ds(j, Q, stride=QROWS)
        row1[every, :] = jnp.broadcast_to(column(fscale_ref[...] * (1.0 / 127.0)), (Q, LANES))
        row2[every, :] = jnp.broadcast_to(column(sscale_ref[...] * (1.0 / 255.0)), (Q, LANES))

    def wide(v):
        return jnp.concatenate([v] * REP, axis=1)

    def piece(block, r):
        return wbuf.at[block, chunk_rows(r), :]

    def pair_weight(c, r, block):
        k = c * NM + r
        return remote(piece(block, r), piece(block, r), wx_send.at[k], wx_recv.at[k], dp=mate)

    def line_weight(c, r, way, to):
        k = c * NM + r
        w = piece(c * B + b, r)
        return remote(w, w, wz_send.at[way * A * NM + k], wz_recv.at[k], dp=to)

    def pair_weight_tail(block):
        return remote(piece(block, tail), piece(block, tail), wxt_sem.at[0], wxt_sem.at[1], dp=mate)

    def line_weight_tail(c, half, way, to):
        k = c * B + half
        return remote(piece(k, tail), piece(k, tail), wt_send.at[way * n + k], wt_recv.at[k], dp=to)

    def weight_out(block):
        at = pl.ds(0, NM * R)
        return pltpu.make_async_copy(wbuf.at[block, at, :], w_hbm.at[block, at, :], wout_sem.at[0, block])

    def weight_tail_out(block):
        return pltpu.make_async_copy(piece(block, tail), w_hbm.at[block, chunk_rows(tail), :], wout_sem.at[1, block])

    def send_own(r):
        @pl.when(a < A - 1)
        def _():
            line_weight(a, r, 0, me + B).start()

        @pl.when(a > 0)
        def _():
            line_weight(a, r, 1, me - B).start()

        pair_weight(a, r, me).start()

    @pl.loop(0, NR)
    def _(k):
        r = (k + NM) % NR
        at = chunk_rows(r)
        clipped = part[at_rows(me, r), :] * factor
        first_new = beta_one * (fc[at, :].astype(jnp.float32) * wide(row1[at, :])) + (1.0 - beta_one) * clipped
        second_new = (
            beta_two * (sc[at, :].astype(jnp.float32) * wide(row2[at, :])) + (1.0 - beta_two) * clipped * clipped
        )
        fn[at, :] = first_new
        sn[at, :] = second_new
        first_hat = first_new * (1.0 / (1.0 - beta_one**STEP))
        second_hat = second_new * (1.0 / (1.0 - beta_two**STEP))
        step_dir = first_hat / (jnp.sqrt(second_hat) + epsilon)
        old = master[at, :]
        new = old - learn_rate * (step_dir + weight_decay * old)
        nm_v[at, :] = new
        wbuf[me, at, :] = new.astype(jnp.bfloat16)

        if NT:

            @pl.when(r == tail)
            def _():
                pair_weight_tail(me).start()

        @pl.when(r < NM)
        def _():
            send_own(r)

    nm_out_copy = pltpu.make_async_copy(nm_v, nm_hbm, out_sem.at[0])
    fu_out_copy = pltpu.make_async_copy(fu_v, fu_hbm, out_sem.at[1])
    su_out_copy = pltpu.make_async_copy(su_v, su_hbm, out_sem.at[2])
    nm_out_copy.start()
    weight_out(me).start()
    if NT:
        weight_tail_out(me).start()

    @pl.loop(0, NR)
    def _(r):
        at = chunk_rows(r)
        row1[at, :] = jnp.broadcast_to(jnp.max(jnp.abs(fn[at, :]), axis=1, keepdims=True), (R, LANES))
        row2[at, :] = jnp.broadcast_to(jnp.max(sn[at, :], axis=1, keepdims=True), (R, LANES))

    for row, top_ref in ((row1, ftop_ref), (row2, stop_ref)):
        top = row[pl.ds(0, Q, stride=QROWS), :]
        for j in range(1, QROWS):
            top = jnp.maximum(top, row[pl.ds(j, Q, stride=QROWS), :])
        top = top + 1e-06
        top_ref[...] = jnp.sum(jnp.where(pick, top[:, :1], 0.0), axis=0, keepdims=True)
        for j in range(QROWS):
            row[pl.ds(j, Q, stride=QROWS), :] = 1.0 / top

    @pl.loop(0, NR)
    def _(r):
        at = chunk_rows(r)
        fu_v[at, :] = fn[at, :] * wide(row1[at, :])
        su_v[at, :] = sn[at, :] * wide(row2[at, :])

    fu_out_copy.start()
    su_out_copy.start()

    sides = ((0, lambda d: a - d, me + B, a < A - 1), (1, lambda d: a + d, me - B, a > 0))

    def inside(c):
        return (c >= 0) & (c < A)

    @pl.loop(1, A)
    def _(d):
        @pl.loop(0, NM)
        def _(r):
            for way, chunk, to, on in sides:
                c = chunk(d)

                @pl.when(inside(c))
                def _():
                    line_weight(c, r, way, me).wait_recv()

                    @pl.when(on)
                    def _():
                        line_weight(c, r, way, to).start()

                    pair_weight(c, r, c * B + b).start()

        for way, chunk, to, on in sides:
            c = chunk(d)

            @pl.when(inside(c))
            def _():
                weight_out(c * B + b).start()

        if NT:

            @pl.when(d == 1)
            def _():
                pair_weight_tail(mate).wait_recv()
                weight_tail_out(mate).start()
                for half in range(B):
                    for way, chunk, to, on in sides:

                        @pl.when(on)
                        def _():
                            line_weight_tail(a, half, way, to).start()

    if NT:

        @pl.loop(1, A)
        def _(d):
            for half in range(B):
                for way, chunk, to, on in sides:
                    c = chunk(d)

                    @pl.when(inside(c))
                    def _():
                        line_weight_tail(c, half, way, me).wait_recv()

                        @pl.when(on)
                        def _():
                            line_weight_tail(c, half, way, to).start()

                        weight_tail_out(c * B + half).start()

    def take_pair(c):
        @pl.loop(0, NM)
        def _(r):
            pair_weight(c, r, c * B + 1 - b).wait_recv()

        weight_out(c * B + 1 - b).start()

    take_pair(a)

    @pl.loop(1, A)
    def _(d):
        for way, chunk, to, on in sides:
            c = chunk(d)

            @pl.when(inside(c))
            def _():
                take_pair(c)

    @pl.loop(0, A)
    def _(c):
        @pl.loop(0, NM)
        def _(r):
            for cp in pair_copies(c, r):
                cp.wait_send()

            @pl.when(c != a)
            def _():
                for cp in line_copies(c, r, 0, me):
                    cp.wait_send()

            pair_weight(c, r, c * B + b).wait_send()

            @pl.when((c <= a) & (a < A - 1))
            def _():
                line_weight(c, r, 0, me).wait_send()

            @pl.when((c >= a) & (a > 0))
            def _():
                line_weight(c, r, 1, me).wait_send()

        if NT:
            for half in range(B):

                @pl.when(c != a)
                def _():
                    for cp in tail_copies(c, half, 0, me):
                        cp.wait_send()

                @pl.when((c <= a) & (a < A - 1))
                def _():
                    line_weight_tail(c, half, 0, me).wait_send()

                @pl.when((c >= a) & (a > 0))
                def _():
                    line_weight_tail(c, half, 1, me).wait_send()

    if NT:
        for cp in pair_tail:
            cp.wait_send()
        pair_weight_tail(me).wait_send()

    @pl.loop(0, n)
    def _(k):
        weight_out(k).wait()
        if NT:
            weight_tail_out(k).wait()

    nm_out_copy.wait()
    fu_out_copy.wait()
    su_out_copy.wait()


def shards(n, m, limit, inputs, key_cotangent, master, first_codes, second_codes, first_scale, second_scale):
    rows, width = master.shape
    tokens, cols = inputs.shape
    A = n // 2
    R = 96 if rows % 96 == 0 else rows
    NR = rows // R
    NM = NR - 1 if NR >= 6 else NR
    Q = rows // QROWS
    f32 = jnp.float32
    any_spec = pl.BlockSpec(memory_space=pl.ANY)
    vmem_spec = pl.BlockSpec(memory_space=pltpu.VMEM)
    dma = pltpu.SemaphoreType.DMA
    block = (rows, width)
    outs = pl.pallas_call(
        functools.partial(kernel, n, m, limit),
        out_shape=(
            jax.ShapeDtypeStruct((n, rows, width), jnp.bfloat16),
            jax.ShapeDtypeStruct(block, f32),
            jax.ShapeDtypeStruct(block, f32),
            jax.ShapeDtypeStruct(block, f32),
            jax.ShapeDtypeStruct((1, Q), f32),
            jax.ShapeDtypeStruct((1, Q), f32),
        ),
        in_specs=[any_spec] * 5 + [vmem_spec] * 2,
        out_specs=[any_spec] * 4 + [vmem_spec] * 2,
        scratch_shapes=[
            pltpu.VMEM((tokens, cols), jnp.bfloat16),
            pltpu.VMEM(key_cotangent.shape, jnp.bfloat16),
            pltpu.VMEM((cols, width), f32),
            pltpu.VMEM((A * NM, R, width), jnp.int16),
            pltpu.VMEM((A * NM, 8, width), f32),
            pltpu.VMEM((A * NM, R, width), jnp.int16),
            pltpu.VMEM((A * NM, 8, width), f32),
            pltpu.VMEM((A * NM, R, width), jnp.int16),
            pltpu.VMEM((A * NM, 8, width), f32),
            pltpu.VMEM((2 * A * NM, R, width), jnp.int16),
            pltpu.VMEM((2 * A * NM, 8, width), f32),
            pltpu.VMEM((n, R, width), jnp.int16),
            pltpu.VMEM((n, 8, width), f32),
            pltpu.VMEM((2 * n, R, width), jnp.int16),
            pltpu.VMEM((2 * n, 8, width), f32),
            pltpu.VMEM((2, R, width), jnp.int16),
            pltpu.VMEM((2, 8, width), f32),
            pltpu.VMEM(block, f32),
            pltpu.VMEM(block, jnp.int32),
            pltpu.VMEM(block, jnp.int32),
            pltpu.VMEM(block, f32),
            pltpu.VMEM(block, f32),
            pltpu.VMEM(block, f32),
            pltpu.VMEM(block, f32),
            pltpu.VMEM(block, f32),
            pltpu.VMEM((rows, LANES), f32),
            pltpu.VMEM((rows, LANES), f32),
            pltpu.VMEM((n, rows, width), jnp.bfloat16),
            pltpu.VMEM((8, LANES), f32),
            pltpu.VMEM((n, 8, LANES), f32),
            pltpu.VMEM((8, LANES), f32),
            pltpu.VMEM((m, 8, LANES), f32),
            dma((A,)),
            dma((4,)),
            dma((A * NM,)),
            dma((A * NM,)),
            dma((A * NM,)),
            dma((A * NM,)),
            dma((A * NM,)),
            dma((2 * A * NM,)),
            dma((A * NM,)),
            dma((2 * A * NM,)),
            dma((2, n)),
            dma((2, 2 * n)),
            dma((4,)),
            dma((n,)),
            dma((n,)),
            dma((m,)),
            dma((m,)),
            dma((A * NM,)),
            dma((A * NM,)),
            dma((2 * A * NM,)),
            dma((A * NM,)),
            dma((2,)),
            dma((2 * n,)),
            dma((n,)),
            dma((2, n)),
            dma((3,)),
        ],
        compiler_params=pltpu.CompilerParams(
            collective_id=0, has_side_effects=True, vmem_limit_bytes=62 * 1024 * 1024
        ),
        name="step",
    )(inputs, key_cotangent, master, first_codes, second_codes, first_scale.reshape(1, Q), second_scale.reshape(1, Q))
    weight = outs[0].reshape(n * rows, width)
    return (weight, *outs[1:4], outs[4].reshape(Q, 1), outs[5].reshape(Q, 1))


def solution(mesh):
    n, m = mesh.shape["dp"], mesh.shape["mp"]

    def run(inputs, key_cotangent, master, *rest):
        limit = clip_rms * math.sqrt(inputs.shape[1] * key_cotangent.shape[1])
        return jax.shard_map(
            functools.partial(shards, n, m, limit),
            mesh=mesh,
            in_specs=(
                P("dp", None),
                P("dp", "mp"),
                P("dp", "mp"),
                P("dp", "mp"),
                P("dp", "mp"),
                P("dp", "mp"),
                P("dp", "mp"),
            ),
            out_specs=(
                P(None, "mp"),
                P("dp", "mp"),
                P("dp", "mp"),
                P("dp", "mp"),
                P("dp", "mp"),
                P("dp", "mp"),
            ),
            check_vma=False,
        )(inputs, key_cotangent, master, *rest)

    return run
```

```python
import functools
import math

import jax
import jax.numpy as jnp
from jax import lax
from jax.experimental import pallas as pl
from jax.experimental.pallas import tpu as pltpu
from jax.sharding import PartitionSpec as P

MESH = pl.DeviceIdType.MESH
QROWS = 4
STEP = 10
LANES = 128

beta_one = 0.9
beta_two = 0.95
learn_rate = 0.002
weight_decay = 0.1
epsilon = 1e-08
clip_rms = 0.25
CODE_MAX = 32767.0


def kernel(
    n,
    m,
    limit,
    x_hbm,
    cot_hbm,
    master_hbm,
    fc_hbm,
    sc_hbm,
    fscale_ref,
    sscale_ref,
    w_hbm,
    nm_hbm,
    fu_hbm,
    su_hbm,
    ftop_ref,
    stop_ref,
    x_v,
    cot_v,
    part,
    xs,
    xs_s,
    xr,
    xr_s,
    zs,
    zs_s,
    zr,
    zr_s,
    zts,
    zts_s,
    ztr,
    ztr_s,
    xt,
    xt_s,
    master,
    fc,
    sc,
    fn,
    sn,
    nm_v,
    fu_v,
    su_v,
    row1,
    row2,
    wbuf,
    nd_out,
    nd_in,
    nm_out,
    nm_in,
    in_sem,
    par_sem,
    xs_send,
    xs_recv,
    xss_send,
    xss_recv,
    zs_send,
    zs_recv,
    zss_send,
    zss_recv,
    zt_send,
    zt_recv,
    xt_sem,
    nd_send,
    nd_recv,
    nmx_send,
    nmx_recv,
    wx_send,
    wx_recv,
    wz_send,
    wz_recv,
    wxt_sem,
    wt_send,
    wt_recv,
    wout_sem,
    out_sem,
):
    B = 2
    A = n // B
    rows, width = master.shape
    cols_total = x_v.shape[1]
    R = 96 if rows % 96 == 0 else rows
    NR = rows // R
    NT = 1 if NR >= 6 else 0
    NM = NR - NT
    tail = NM
    Q = rows // QROWS
    REP = width // LANES

    me = lax.axis_index("dp")
    my = lax.axis_index("mp")
    a = me // B
    b = me % B
    mate = a * B + (1 - b)

    hi = A - 1 - a
    lo = a
    up_longer = jnp.where(hi >= lo, 1, -1)
    short = jnp.minimum(hi, lo)
    long = jnp.maximum(hi, lo)

    def order(i):
        j = i - (long - short)
        d_far = long - i
        jj = jnp.maximum(j, 0)
        d_near = short - jj // 2
        sgn = jnp.where(jj % 2 == 0, up_longer, -up_longer)
        return jnp.where(j < 0, a + up_longer * d_far, a + sgn * d_near)

    per_chunk = (B * rows) % 384 == 0
    csize = B * rows

    def in_copy(c):
        if per_chunk:
            sl = pl.ds(pl.multiple_of(c * csize, LANES), csize)
            return pltpu.make_async_copy(x_hbm.at[:, sl], x_v.at[:, sl], in_sem.at[c])
        return pltpu.make_async_copy(x_hbm, x_v, in_sem.at[0])

    cot_copy = pltpu.make_async_copy(cot_hbm, cot_v, par_sem.at[0])
    par_copies = [
        pltpu.make_async_copy(src, dst, par_sem.at[k + 1])
        for k, (src, dst) in enumerate(((master_hbm, master), (fc_hbm, fc), (sc_hbm, sc)))
    ]
    cot_copy.start()
    in_copy(order(0) if per_chunk else 0).start()

    barrier = pltpu.get_barrier_semaphore()

    @pl.loop(1, n)
    def _(k):
        pl.semaphore_signal(barrier, inc=1, device_id={"dp": (me + k) % n}, device_id_type=MESH)

    @pl.loop(1, m)
    def _(k):
        pl.semaphore_signal(barrier, inc=1, device_id={"mp": (my + k) % m}, device_id_type=MESH)

    def multiply(first, count):
        @pl.loop(0, count)
        def _(k):
            at = pl.ds(pl.multiple_of(first + k * 384, LANES), 384)
            part[at, :] = lax.dot_general(
                x_v[:, at], cot_v[...], (((0,), (0,)), ((), ())), preferred_element_type=jnp.float32
            )

    def at_rows(block, r):
        return pl.ds(pl.multiple_of(block * rows + r * R, 8), R)

    def chunk_rows(r):
        return pl.ds(pl.multiple_of(r * R, 8), R)

    def fold(v):
        return v.reshape(R // 8, 8, width)

    def encode(block, r, dst, dst_s):
        v = part[at_rows(block, r), :]
        top = jnp.max(jnp.max(jnp.abs(fold(v)), axis=0), axis=0, keepdims=True)
        top = jnp.maximum(top, 1e-30)
        dst_s[...] = top * (1.0 / CODE_MAX)
        v = jnp.round(v * (CODE_MAX / top))
        dst[...] = v.astype(jnp.int32).astype(jnp.int16)

    def decode(src, src_s):
        return src[...].astype(jnp.int32).astype(jnp.float32) * src_s[...]

    def add(block, r, src, src_s):
        at = at_rows(block, r)
        part[at, :] = part[at, :] + decode(src, src_s)

    def remote(src, dst, send, recv, **to):
        return pltpu.make_async_remote_copy(src, dst, send, recv, device_id=to, device_id_type=MESH)

    def pair_copies(c, r):
        k = c * NM + r
        return (
            remote(xs.at[k], xr.at[k], xs_send.at[k], xs_recv.at[k], dp=mate),
            remote(xs_s.at[k], xr_s.at[k], xss_send.at[k], xss_recv.at[k], dp=mate),
        )

    def line_copies(c, r, way, to):
        k = c * NM + r
        t = (way * A + c) * NM + r
        return (
            remote(zs.at[k], zr.at[t], zs_send.at[k], zs_recv.at[t], dp=to),
            remote(zs_s.at[k], zr_s.at[t], zss_send.at[k], zss_recv.at[t], dp=to),
        )

    def tail_copies(c, half, way, to):
        k = c * B + half
        t = (way * A + c) * B + half
        return (
            remote(zts.at[k], ztr.at[t], zt_send.at[0, k], zt_recv.at[0, t], dp=to),
            remote(zts_s.at[k], ztr_s.at[t], zt_send.at[1, k], zt_recv.at[1, t], dp=to),
        )

    pair_tail = (
        remote(xt.at[0], xt.at[1], xt_sem.at[0], xt_sem.at[1], dp=mate),
        remote(xt_s.at[0], xt_s.at[1], xt_sem.at[2], xt_sem.at[3], dp=mate),
    )

    cot_copy.wait()
    if not per_chunk:
        in_copy(0).wait()
        multiply(0, cols_total // 384)

    def send_tail(c):
        for way, on, to in ((0, c > a, me + B), (1, c < a, me - B)):

            @pl.when(on)
            def _():
                for half in range(B):
                    k = c * B + half
                    encode(k, tail, zts.at[k], zts_s.at[k])
                    for cp in tail_copies(c, half, way, to):
                        cp.start()

    def receive_tail(c, way):
        for half in range(B):
            t = (way * A + c) * B + half
            for cp in tail_copies(c, half, way, me):
                cp.wait_recv()
            add(c * B + half, tail, ztr.at[t], ztr_s.at[t])

    def starts(c):
        return ((c > a) & (a == 0)) | ((c < a) & (a == A - 1))

    @pl.loop(0, A)
    def _(i):
        c = order(i)
        if per_chunk:
            in_copy(c).wait()

            @pl.when(i < A - 1)
            def _():
                in_copy(order(i + 1)).start()

            multiply(c * csize, csize // 384)
        block = c * B + (1 - b)

        @pl.when(i == 0)
        def _():
            pl.semaphore_wait(barrier, n - 1 + m - 1)

        @pl.loop(0, NM)
        def _(r):
            k = c * NM + r
            encode(block, r, xs.at[k], xs_s.at[k])
            for cp in pair_copies(c, r):
                cp.start()

        if NT:

            @pl.when(starts(c))
            def _():
                send_tail(c)

    for cp in par_copies:
        cp.start()

    def receive(c, r, way):
        t = (way * A + c) * NM + r
        for cp in line_copies(c, r, way, me):
            cp.wait_recv()
        add(c * B + b, r, zr.at[t], zr_s.at[t])

    def forward(c, r, way, to):
        k = c * NM + r
        encode(c * B + b, r, zs.at[k], zs_s.at[k])
        for cp in line_copies(c, r, way, to):
            cp.start()

    @pl.loop(0, A)
    def _(i):
        c = order(i)
        if NT:
            for way, on in ((0, (c >= a) & (a > 0)), (1, (c <= a) & (a < A - 1))):

                @pl.when(on)
                def _():
                    receive_tail(c, way)

            @pl.when((c != a) & jnp.logical_not(starts(c)))
            def _():
                send_tail(c)

            @pl.when(c == a)
            def _():
                encode(mate, tail, xt.at[0], xt_s.at[0])
                for cp in pair_tail:
                    cp.start()

        @pl.loop(0, NM)
        def _(r):
            k = c * NM + r
            for cp in pair_copies(c, r):
                cp.wait_recv()
            add(c * B + b, r, xr.at[k], xr_s.at[k])

            for way, on in ((0, (c >= a) & (a > 0)), (1, (c <= a) & (a < A - 1))):

                @pl.when(on)
                def _():
                    receive(c, r, way)

            for way, on, to in ((0, c > a, me + B), (1, c < a, me - B)):

                @pl.when(on)
                def _():
                    forward(c, r, way, to)

    if NT:
        for cp in pair_tail:
            cp.wait_recv()
        add(me, tail, xt.at[1], xt_s.at[1])

    def square(r, t):
        g = fold(part[at_rows(me, r), :])
        return t + jnp.sum(g * g, axis=0)

    squares = lax.fori_loop(0, NR, square, jnp.zeros((8, width), jnp.float32))
    mine = squares[:, :LANES]
    for k in range(1, REP):
        mine = mine + squares[:, k * LANES : (k + 1) * LANES]

    def exchange(axis, size, own, value, out, inbox, send, recv):
        out[...] = value
        inbox[own] = value

        def copy(k, slot):
            return pltpu.make_async_remote_copy(
                out,
                inbox.at[slot],
                send.at[k],
                recv.at[slot],
                device_id={axis: (own + k) % size},
                device_id_type=MESH,
            )

        @pl.loop(1, size)
        def _(k):
            copy(k, own).start()

        @pl.loop(1, size)
        def _(k):
            copy(k, (own + k) % size).wait_recv()

        @pl.loop(1, size)
        def _(k):
            copy(k, own).wait_send()

        return jnp.sum(inbox[...], axis=0)

    over_dp = exchange("dp", n, me, mine, nd_out, nd_in, nd_send, nd_recv)
    over_all = exchange("mp", m, my, over_dp, nm_out, nm_in, nmx_send, nmx_recv)
    norm_sq = jnp.sum(jnp.sum(over_all, axis=0, keepdims=True), axis=1, keepdims=True)
    factor = jnp.minimum(1.0, limit / (jnp.sqrt(norm_sq) + 1e-06))

    for cp in par_copies:
        cp.wait()
    pick = lax.broadcasted_iota(jnp.int32, (Q, Q), 0) == lax.broadcasted_iota(jnp.int32, (Q, Q), 1)

    def column(row):
        return jnp.sum(jnp.where(pick, row, 0.0), axis=1, keepdims=True)

    for j in range(QROWS):
        every = pl.ds(j, Q, stride=QROWS)
        row1[every, :] = jnp.broadcast_to(column(fscale_ref[...] * (1.0 / 127.0)), (Q, LANES))
        row2[every, :] = jnp.broadcast_to(column(sscale_ref[...] * (1.0 / 255.0)), (Q, LANES))

    def wide(v):
        return jnp.concatenate([v] * REP, axis=1)

    def piece(block, r):
        return wbuf.at[block, chunk_rows(r), :]

    def pair_weight(c, r, block):
        k = c * NM + r
        return remote(piece(block, r), piece(block, r), wx_send.at[k], wx_recv.at[k], dp=mate)

    def line_weight(c, r, way, to):
        k = c * NM + r
        w = piece(c * B + b, r)
        return remote(w, w, wz_send.at[way * A * NM + k], wz_recv.at[k], dp=to)

    def pair_weight_tail(block):
        return remote(piece(block, tail), piece(block, tail), wxt_sem.at[0], wxt_sem.at[1], dp=mate)

    def line_weight_tail(c, half, way, to):
        k = c * B + half
        return remote(piece(k, tail), piece(k, tail), wt_send.at[way * n + k], wt_recv.at[k], dp=to)

    def weight_out(block):
        at = pl.ds(0, NM * R)
        return pltpu.make_async_copy(wbuf.at[block, at, :], w_hbm.at[block, at, :], wout_sem.at[0, block])

    def weight_tail_out(block):
        return pltpu.make_async_copy(piece(block, tail), w_hbm.at[block, chunk_rows(tail), :], wout_sem.at[1, block])

    def send_own(r):
        @pl.when(a < A - 1)
        def _():
            line_weight(a, r, 0, me + B).start()

        @pl.when(a > 0)
        def _():
            line_weight(a, r, 1, me - B).start()

        pair_weight(a, r, me).start()

    @pl.loop(0, NR)
    def _(k):
        r = (k + NM) % NR
        at = chunk_rows(r)
        clipped = part[at_rows(me, r), :] * factor
        first_new = beta_one * (fc[at, :].astype(jnp.float32) * wide(row1[at, :])) + (1.0 - beta_one) * clipped
        second_new = (
            beta_two * (sc[at, :].astype(jnp.float32) * wide(row2[at, :])) + (1.0 - beta_two) * clipped * clipped
        )
        fn[at, :] = first_new
        sn[at, :] = second_new
        first_hat = first_new * (1.0 / (1.0 - beta_one**STEP))
        second_hat = second_new * (1.0 / (1.0 - beta_two**STEP))
        step_dir = first_hat / (jnp.sqrt(second_hat) + epsilon)
        old = master[at, :]
        new = old - learn_rate * (step_dir + weight_decay * old)
        nm_v[at, :] = new
        wbuf[me, at, :] = new.astype(jnp.bfloat16)

        if NT:

            @pl.when(r == tail)
            def _():
                pair_weight_tail(me).start()

        @pl.when(r < NM)
        def _():
            send_own(r)

    nm_out_copy = pltpu.make_async_copy(nm_v, nm_hbm, out_sem.at[0])
    fu_out_copy = pltpu.make_async_copy(fu_v, fu_hbm, out_sem.at[1])
    su_out_copy = pltpu.make_async_copy(su_v, su_hbm, out_sem.at[2])
    nm_out_copy.start()
    weight_out(me).start()
    if NT:
        weight_tail_out(me).start()

    @pl.loop(0, NR)
    def _(r):
        at = chunk_rows(r)
        row1[at, :] = jnp.broadcast_to(jnp.max(jnp.abs(fn[at, :]), axis=1, keepdims=True), (R, LANES))
        row2[at, :] = jnp.broadcast_to(jnp.max(sn[at, :], axis=1, keepdims=True), (R, LANES))

    for row, top_ref in ((row1, ftop_ref), (row2, stop_ref)):
        top = row[pl.ds(0, Q, stride=QROWS), :]
        for j in range(1, QROWS):
            top = jnp.maximum(top, row[pl.ds(j, Q, stride=QROWS), :])
        top = top + 1e-06
        top_ref[...] = jnp.sum(jnp.where(pick, top[:, :1], 0.0), axis=0, keepdims=True)
        for j in range(QROWS):
            row[pl.ds(j, Q, stride=QROWS), :] = 1.0 / top

    @pl.loop(0, NR)
    def _(r):
        at = chunk_rows(r)
        fu_v[at, :] = fn[at, :] * wide(row1[at, :])
        su_v[at, :] = sn[at, :] * wide(row2[at, :])

    fu_out_copy.start()
    su_out_copy.start()

    sides = ((0, lambda d: a - d, me + B, a < A - 1), (1, lambda d: a + d, me - B, a > 0))

    def inside(c):
        return (c >= 0) & (c < A)

    @pl.loop(1, A)
    def _(d):
        @pl.loop(0, NM)
        def _(r):
            for way, chunk, to, on in sides:
                c = chunk(d)

                @pl.when(inside(c))
                def _():
                    line_weight(c, r, way, me).wait_recv()

                    @pl.when(on)
                    def _():
                        line_weight(c, r, way, to).start()

                    pair_weight(c, r, c * B + b).start()

        for way, chunk, to, on in sides:
            c = chunk(d)

            @pl.when(inside(c))
            def _():
                weight_out(c * B + b).start()

        if NT:

            @pl.when(d == 1)
            def _():
                pair_weight_tail(mate).wait_recv()
                weight_tail_out(mate).start()
                for half in range(B):
                    for way, chunk, to, on in sides:

                        @pl.when(on)
                        def _():
                            line_weight_tail(a, half, way, to).start()

    if NT:

        @pl.loop(1, A)
        def _(d):
            for half in range(B):
                for way, chunk, to, on in sides:
                    c = chunk(d)

                    @pl.when(inside(c))
                    def _():
                        line_weight_tail(c, half, way, me).wait_recv()

                        @pl.when(on)
                        def _():
                            line_weight_tail(c, half, way, to).start()

                        weight_tail_out(c * B + half).start()

    def take_pair(c):
        @pl.loop(0, NM)
        def _(r):
            pair_weight(c, r, c * B + 1 - b).wait_recv()

        weight_out(c * B + 1 - b).start()

    take_pair(a)

    @pl.loop(1, A)
    def _(d):
        for way, chunk, to, on in sides:
            c = chunk(d)

            @pl.when(inside(c))
            def _():
                take_pair(c)

    @pl.loop(0, A)
    def _(c):
        @pl.loop(0, NM)
        def _(r):
            for cp in pair_copies(c, r):
                cp.wait_send()

            @pl.when(c != a)
            def _():
                for cp in line_copies(c, r, 0, me):
                    cp.wait_send()

            pair_weight(c, r, c * B + b).wait_send()

            @pl.when((c <= a) & (a < A - 1))
            def _():
                line_weight(c, r, 0, me).wait_send()

            @pl.when((c >= a) & (a > 0))
            def _():
                line_weight(c, r, 1, me).wait_send()

        if NT:
            for half in range(B):

                @pl.when(c != a)
                def _():
                    for cp in tail_copies(c, half, 0, me):
                        cp.wait_send()

                @pl.when((c <= a) & (a < A - 1))
                def _():
                    line_weight_tail(c, half, 0, me).wait_send()

                @pl.when((c >= a) & (a > 0))
                def _():
                    line_weight_tail(c, half, 1, me).wait_send()

    if NT:
        for cp in pair_tail:
            cp.wait_send()
        pair_weight_tail(me).wait_send()

    @pl.loop(0, n)
    def _(k):
        weight_out(k).wait()
        if NT:
            weight_tail_out(k).wait()

    nm_out_copy.wait()
    fu_out_copy.wait()
    su_out_copy.wait()


def shards(n, m, limit, inputs, key_cotangent, master, first_codes, second_codes, first_scale, second_scale):
    rows, width = master.shape
    tokens, cols = inputs.shape
    A = n // 2
    R = 96 if rows % 96 == 0 else rows
    NR = rows // R
    NM = NR - 1 if NR >= 6 else NR
    Q = rows // QROWS
    f32 = jnp.float32
    any_spec = pl.BlockSpec(memory_space=pl.ANY)
    vmem_spec = pl.BlockSpec(memory_space=pltpu.VMEM)
    dma = pltpu.SemaphoreType.DMA
    block = (rows, width)
    outs = pl.pallas_call(
        functools.partial(kernel, n, m, limit),
        out_shape=(
            jax.ShapeDtypeStruct((n, rows, width), jnp.bfloat16),
            jax.ShapeDtypeStruct(block, f32),
            jax.ShapeDtypeStruct(block, f32),
            jax.ShapeDtypeStruct(block, f32),
            jax.ShapeDtypeStruct((1, Q), f32),
            jax.ShapeDtypeStruct((1, Q), f32),
        ),
        in_specs=[any_spec] * 5 + [vmem_spec] * 2,
        out_specs=[any_spec] * 4 + [vmem_spec] * 2,
        scratch_shapes=[
            pltpu.VMEM((tokens, cols), jnp.bfloat16),
            pltpu.VMEM(key_cotangent.shape, jnp.bfloat16),
            pltpu.VMEM((cols, width), f32),
            pltpu.VMEM((A * NM, R, width), jnp.int16),
            pltpu.VMEM((A * NM, 1, width), f32),
            pltpu.VMEM((A * NM, R, width), jnp.int16),
            pltpu.VMEM((A * NM, 1, width), f32),
            pltpu.VMEM((A * NM, R, width), jnp.int16),
            pltpu.VMEM((A * NM, 1, width), f32),
            pltpu.VMEM((2 * A * NM, R, width), jnp.int16),
            pltpu.VMEM((2 * A * NM, 1, width), f32),
            pltpu.VMEM((n, R, width), jnp.int16),
            pltpu.VMEM((n, 1, width), f32),
            pltpu.VMEM((2 * n, R, width), jnp.int16),
            pltpu.VMEM((2 * n, 1, width), f32),
            pltpu.VMEM((2, R, width), jnp.int16),
            pltpu.VMEM((2, 1, width), f32),
            pltpu.VMEM(block, f32),
            pltpu.VMEM(block, jnp.int32),
            pltpu.VMEM(block, jnp.int32),
            pltpu.VMEM(block, f32),
            pltpu.VMEM(block, f32),
            pltpu.VMEM(block, f32),
            pltpu.VMEM(block, f32),
            pltpu.VMEM(block, f32),
            pltpu.VMEM((rows, LANES), f32),
            pltpu.VMEM((rows, LANES), f32),
            pltpu.VMEM((n, rows, width), jnp.bfloat16),
            pltpu.VMEM((8, LANES), f32),
            pltpu.VMEM((n, 8, LANES), f32),
            pltpu.VMEM((8, LANES), f32),
            pltpu.VMEM((m, 8, LANES), f32),
            dma((A,)),
            dma((4,)),
            dma((A * NM,)),
            dma((A * NM,)),
            dma((A * NM,)),
            dma((A * NM,)),
            dma((A * NM,)),
            dma((2 * A * NM,)),
            dma((A * NM,)),
            dma((2 * A * NM,)),
            dma((2, n)),
            dma((2, 2 * n)),
            dma((4,)),
            dma((n,)),
            dma((n,)),
            dma((m,)),
            dma((m,)),
            dma((A * NM,)),
            dma((A * NM,)),
            dma((2 * A * NM,)),
            dma((A * NM,)),
            dma((2,)),
            dma((2 * n,)),
            dma((n,)),
            dma((2, n)),
            dma((3,)),
        ],
        compiler_params=pltpu.CompilerParams(
            collective_id=0, has_side_effects=True, vmem_limit_bytes=62 * 1024 * 1024
        ),
        name="step",
    )(inputs, key_cotangent, master, first_codes, second_codes, first_scale.reshape(1, Q), second_scale.reshape(1, Q))
    weight = outs[0].reshape(n * rows, width)
    return (weight, *outs[1:4], outs[4].reshape(Q, 1), outs[5].reshape(Q, 1))


def solution(mesh):
    n, m = mesh.shape["dp"], mesh.shape["mp"]

    def run(inputs, key_cotangent, master, *rest):
        limit = clip_rms * math.sqrt(inputs.shape[1] * key_cotangent.shape[1])
        return jax.shard_map(
            functools.partial(shards, n, m, limit),
            mesh=mesh,
            in_specs=(
                P("dp", None),
                P("dp", "mp"),
                P("dp", "mp"),
                P("dp", "mp"),
                P("dp", "mp"),
                P("dp", "mp"),
                P("dp", "mp"),
            ),
            out_specs=(
                P(None, "mp"),
                P("dp", "mp"),
                P("dp", "mp"),
                P("dp", "mp"),
                P("dp", "mp"),
                P("dp", "mp"),
            ),
            check_vma=False,
        )(inputs, key_cotangent, master, *rest)

    return run
```
